32 devices in a mesh: dp: 16 (over z, y, x), mp: 2 (over core).
Axes of the slice: x: 2, y: 2, z: 4, core: 2. Of those that a mesh axis runs over, the one named last changes fastest.
Arguments:
- tokens: bfloat16 [20480, 1024], P('dp'), may hold values from -6 to 6
- image_class: int32 [240], P('dp'), may hold values from 0 to 1, as said below
- interp_index: int32 [145, 4], replicated, may hold values from 0 to 49
- interp_weight: int32 [145, 4], replicated, may hold values from 1 to 16
- position_table: bfloat16 [50, 1024], replicated, may hold values from -3 to 3
- norm_gain: bfloat16 [2, 1024], replicated, may hold values from 0.25 to 1.75
- norm_shift: bfloat16 [2, 1024], replicated, may hold values from -2 to 2
- attn_in_weight: bfloat16 [3, 1024, 1024], P(None, None, 'mp'), may hold values from -0.1875 to 0.1875
- attn_in_bias: bfloat16 [2, 1024], P(None, 'mp'), may hold values from -2 to 2
- attn_out_weight: bfloat16 [1024, 1024], P('mp'), may hold values from -0.75 to 0.75
- attn_out_bias: bfloat16 [1024], replicated, may hold values from -2 to 2
- up_weight: bfloat16 [1024, 4096], P(None, 'mp'), may hold values from -0.1875 to 0.1875
- up_bias: bfloat16 [4096], P('mp'), may hold values from -3 to 3
- down_weight: bfloat16 [4096, 1024], P('mp'), may hold values from -0.125 to 0.125
- down_bias: bfloat16 [1024], replicated, may hold values from -2 to 2
- cotangent: bfloat16 [20480, 1024], P('dp'), may hold values from -6 to 6
Outputs:
- block_out: bfloat16 [20480, 1024], P('dp')
- grad_inputs: float32 [20480, 1024], P('dp')
- grad_table: float32 [50, 1024], replicated
- grad_gain: float32 [2, 1024], replicated
- grad_shift: float32 [2, 1024], replicated
- grad_attn_in: float32 [3, 1024, 1024], P(None, None, 'mp')
- grad_in_bias: float32 [2, 1024], P(None, 'mp')
- grad_attn_out: float32 [1024, 1024], P('mp')
- grad_out_bias: float32 [1024], replicated
- grad_up_proj: float32 [1024, 4096], P(None, 'mp')
- grad_up_bias: float32 [4096], P('mp')
- grad_down_proj: float32 [4096, 1024], P('mp')
- grad_down_bias: float32 [1024], replicated
The draws below stay inside these ranges and needn't reach their ends.
Inputs may be any that keep to these rules, and one draw needn't show every extreme that they name: `image_class`: in the 15 image slots of one index of dp at most 5 are 384px images, and in at least one index exactly 5.
All inputs are finite; a program needn't handle non-finite values.
Results may differ from the reference program's by a relative error of at most 0.012.
The reference program's roundings to bfloat16 on the way count: a program that leaves them out, or rounds other values in their place, can miss the bound.
Values sent between devices are 32-bit elements; how exact they have to be, the bound alone decides.
A program may use at most 320 MiB of HBM per device.

```python
import jax
import jax.numpy as jnp
from jax import lax

D = 1024
HEADS = 16
HD = 64
FF = 4096
POS = 50
LONG = 145
IMG_DEV = 15
BIG_DEV = 5
TOK_DEV = 1280
NIMG = 240
TOKENS = 20480
N_DP = 16


def draw_image_class(key, part):
    devices = NIMG // IMG_DEV
    key_counts, key_busy, key_order = jax.random.split(key, 3)
    counts = jax.random.randint(key_counts, (devices,), 0, BIG_DEV + 1)
    busiest = jax.random.randint(key_busy, (), 0, devices)
    counts = jnp.where(jnp.arange(devices) == busiest, BIG_DEV, counts)
    orders = jax.vmap(lambda subkey: jax.random.permutation(subkey, IMG_DEV))(jax.random.split(key_order, devices))
    return (orders < counts[:, None]).astype(jnp.int32).reshape(NIMG)


def touch_ends(entries, rng, smallest, largest):
    shape = entries.shape
    spot = [jax.random.randint(jax.random.fold_in(rng, axis), (), 0, shape[axis]) for axis in range(len(shape))]
    entries = entries.at[tuple(spot)].set(smallest)
    longest = shape.index(max(shape))
    spot[longest] = (spot[longest] + 1) % shape[longest]
    return entries.at[tuple(spot)].set(largest)


def steps_of(rng, extent, shards, low, largest):
    factor_of, own = 1.0, jax.random.fold_in(rng, 6)
    for dim, parts in shards:
        heights = jnp.exp(jax.random.uniform(jax.random.fold_in(own, dim), (parts,), jnp.float32, low / len(shards), largest / len(shards)))
        factor_of = factor_of * jnp.repeat(heights, extent[dim] // parts).reshape([-1 if axis == dim else 1 for axis in range(len(extent))])
    return factor_of


def scatter_about(stream_key, extent, deviation, bound, cuts=(), kind=jnp.bfloat16):
    values = jax.random.normal(stream_key, extent, jnp.float32) * deviation
    if len(cuts) > 0:
        values = steps_of(stream_key, extent, cuts, -0.22, 0.18) * values
    return jnp.clip(values, min=-bound, max=bound).astype(kind)


def setup_inputs(seed: int = 0) -> dict:
    splits = jax.random.split(jax.random.key(seed), 17)
    tokens = scatter_about(splits[0], (TOKENS, D), 1.0, 6.0, ((0, 16),))
    image_class = draw_image_class(jax.random.fold_in(splits[16], 71), 0)
    interp_index = touch_ends(jax.random.randint(splits[2], (LONG, 4), 0, POS), jax.random.fold_in(splits[2], 1), 0, POS - 1).astype(jnp.int32)
    interp_weight = touch_ends(jax.random.randint(splits[3], (LONG, 4), 1, 17), jax.random.fold_in(splits[3], 1), 1, 16).astype(jnp.int32)
    position_table = scatter_about(splits[4], (POS, D), 0.5, 3.0)
    norm_gain = jnp.clip(1.0 + 0.15 * jax.random.normal(splits[5], (2, D), jnp.float32), 0.25, 1.75).astype(jnp.bfloat16)
    norm_shift = scatter_about(splits[6], (2, D), 0.3, 2.0)
    attn_in_weight = scatter_about(splits[7], (3, D, D), D ** -0.5, 0.1875, ((2, 2),))
    attn_in_bias = scatter_about(splits[8], (2, D), 0.3, 2.0, ((1, 2),))
    attn_out_weight = scatter_about(splits[9], (D, D), (D // 16) ** -0.5, 0.75, ((0, 2),))
    attn_out_bias = scatter_about(splits[10], (D,), 0.3, 2.0)
    up_weight = scatter_about(splits[11], (D, FF), D ** -0.5, 0.1875, ((1, 2),))
    up_bias = scatter_about(splits[12], (FF,), 0.5, 3.0, ((0, 2),))
    down_weight = scatter_about(splits[13], (FF, D), (FF // 2) ** -0.5, 0.125, ((0, 2),))
    down_bias = scatter_about(splits[14], (D,), 0.3, 2.0)
    cotangent = scatter_about(splits[15], (TOKENS, D), 1.0, 6.0, ((0, 16),))
    return {"tokens": tokens, "image_class": image_class, "interp_index": interp_index, "interp_weight": interp_weight, "position_table": position_table, "norm_gain": norm_gain, "norm_shift": norm_shift, "attn_in_weight": attn_in_weight, "attn_in_bias": attn_in_bias, "attn_out_weight": attn_out_weight, "attn_out_bias": attn_out_bias, "up_weight": up_weight, "up_bias": up_bias, "down_weight": down_weight, "down_bias": down_bias, "cotangent": cotangent}


@jax.custom_vjp
def low(v):
    return lax.optimization_barrier(v.astype(jnp.bfloat16)).astype(jnp.float32)

@jax.custom_vjp
def low_back(v):
    return v

def low_keep(v):
    return (low(v), None)

def low_pass(kept, grad):
    return (grad,)

def back_keep(v):
    return (v, None)

def back_low(kept, grad):
    return (low(grad),)
low.defvjp(low_keep, low_pass)
low_back.defvjp(back_keep, back_low)

def layer_norm(inputs, gain_row, shift_row):
    center = inputs - lax.optimization_barrier(jnp.mean(inputs, axis=-1, keepdims=True))
    spread = lax.optimization_barrier(jnp.mean(center * center, axis=-1, keepdims=True))
    return center * lax.rsqrt(spread + 1e-06) * gain_row + shift_row

def exact_gelu(inputs):
    return jax.nn.gelu(inputs, approximate=False)

def token_layout(classes, interp_index, interp_weight, row_count):
    image_count = classes.shape[0]
    lengths = (POS + (LONG - POS) * classes).astype(jnp.int32)
    image_ends = jnp.cumsum(lengths).astype(jnp.int32)
    image_starts = image_ends - lengths
    places = jnp.arange(row_count, dtype=jnp.int32)
    segment = lax.optimization_barrier(jnp.sum((places[:, None] >= image_ends[None, :]).astype(jnp.int32), axis=1)).astype(jnp.int32)
    member = segment[:, None] == jnp.arange(image_count, dtype=jnp.int32)[None, :]
    offset = places - lax.optimization_barrier(jnp.sum(jnp.where(member, image_starts[None, :], 0), axis=1)).astype(jnp.int32)
    is_long = lax.optimization_barrier(jnp.sum(jnp.where(member, classes[None, :], 0), axis=1)).astype(jnp.int32)
    in_image = segment < image_count
    weight_float = interp_weight.astype(jnp.float32)
    weight_share = weight_float / lax.optimization_barrier(jnp.sum(weight_float, axis=1, keepdims=True))
    table_rows = jnp.arange(POS, dtype=jnp.int32)
    long_map = lax.optimization_barrier(jnp.sum(weight_share[:, :, None] * (interp_index[:, :, None] == table_rows[None, None, :]).astype(jnp.float32), axis=1))
    short_pick = ((offset[:, None] == table_rows[None, :]) & in_image[:, None] & (is_long[:, None] == 0)).astype(jnp.float32)
    long_places = jnp.arange(LONG, dtype=jnp.int32)
    long_pick = ((offset[:, None] == long_places[None, :]) & in_image[:, None] & (is_long[:, None] == 1)).astype(jnp.float32)
    mixing = short_pick + jnp.dot(long_pick, long_map, precision=lax.Precision.HIGHEST)
    return (mixing, segment)

def reference(tokens, image_class, interp_index, interp_weight, position_table, norm_gain, norm_shift, attn_in_weight, attn_in_bias, attn_out_weight, attn_out_bias, up_weight, up_bias, down_weight, down_bias, cotangent):
    highest = lax.Precision.HIGHEST
    classes = image_class.reshape(N_DP, IMG_DEV)
    mixing, segment = jax.vmap(lambda block: token_layout(block, interp_index, interp_weight, TOK_DEV))(classes)
    same_image = segment[:, :, None] == segment[:, None, :]
    score_scale = HD ** (-0.5)

    def attend(pieces):
        queries, keys_all, values_all, mask_block = pieces
        scores = low_back(jnp.einsum('qhd,khd->hqk', queries, keys_all, precision=highest) * score_scale)
        scores = jnp.where(mask_block[None], scores, -1000000000.0)
        weights_all = low(jax.nn.softmax(scores, axis=-1))
        return jnp.einsum('hqk,khd->qhd', weights_all, values_all, precision=highest)

    def forward(inputs, table, gains, shifts, in_weight, in_bias, out_weight, out_bias, up_matrix, up_shift, down_matrix, down_shift):
        residual_in = inputs + jnp.einsum('ntp,pd->ntd', mixing, table, precision=highest).reshape(inputs.shape)
        normed_one = low(layer_norm(residual_in, gains[0], shifts[0]))
        projected = jnp.einsum('td,cde->cte', normed_one, in_weight, precision=highest)
        queries = low_back(low(projected[0] + in_bias[0]))
        keys_all = low_back(low(projected[1]))
        values_all = low_back(low(projected[2] + in_bias[1]))
        shaped = (N_DP, TOK_DEV, HEADS, HD)
        attended = lax.map(jax.checkpoint(attend), (queries.reshape(shaped), keys_all.reshape(shaped), values_all.reshape(shaped), same_image))
        attended = low_back(low(attended.reshape(inputs.shape)))
        middle = residual_in + low_back(jnp.dot(attended, out_weight, precision=highest)) + out_bias
        normed_two = low(layer_norm(middle, gains[1], shifts[1]))
        hidden_pre = low_back(jnp.dot(normed_two, up_matrix, precision=highest) + up_shift)
        activ = low(exact_gelu(hidden_pre))
        return middle + low_back(jnp.dot(activ, down_matrix, precision=highest)) + down_shift
    floats = (tokens, position_table, norm_gain, norm_shift, attn_in_weight, attn_in_bias, attn_out_weight, attn_out_bias, up_weight, up_bias, down_weight, down_bias)
    floats = tuple((item.astype(jnp.float32) for item in floats))
    result, backward = jax.vjp(forward, *floats)
    grads = backward(cotangent.astype(jnp.float32))
    return (result.astype(jnp.bfloat16), grads[0], grads[1], grads[2], grads[3], grads[4], grads[5], grads[6], grads[7], grads[8], grads[9], grads[10], grads[11])
```

```python
import jax
import jax.numpy as jnp
from jax import lax
from jax.sharding import PartitionSpec as P

HD = 64
POS = 50
LONG = 145

def log_two(size):
    return size.bit_length() - 1


def swap_pairs(size, bit):
    return [(index, index ^ (1 << bit)) for index in range(size)]


def sum_over(value, axis):
    size = lax.axis_size(axis)
    if size & (size - 1):
        return lax.psum(value, axis)
    for bit in range(log_two(size)):
        value = value + lax.ppermute(value, axis, swap_pairs(size, bit))
    return value


def bit_of(axis, bit):
    return (lax.axis_index(axis) >> bit) & 1


def sum_rows(part, rows, order, axis):
    size = lax.axis_size(axis)
    half = rows // 2
    first = bit_of(axis, order[0])
    sent = part((1 - first) * half, half)
    arrived = lax.ppermute(sent, axis, swap_pairs(size, order[0]))
    held = part(first * half, half)
    for bit in order[1:]:
        half = half // 2
        here = bit_of(axis, bit)
        away = (1 - here) * half
        mine = here * half
        sent = lax.dynamic_slice_in_dim(held, away, half) + lax.dynamic_slice_in_dim(
            arrived, away, half
        )
        held = lax.dynamic_slice_in_dim(held, mine, half) + lax.dynamic_slice_in_dim(
            arrived, mine, half
        )
        arrived = lax.ppermute(sent, axis, swap_pairs(size, bit))
    held = held + arrived
    for bit in reversed(order):
        other = lax.ppermute(held, axis, swap_pairs(size, bit))
        here = bit_of(axis, bit)
        held = jnp.where(
            here == 0,
            jnp.concatenate([held, other], axis=0),
            jnp.concatenate([other, held], axis=0),
        )
    return held


def orders_of(size):
    bits = list(range(log_two(size)))
    return (
        bits,
        [bits[1], bits[0]] + bits[2:],
        bits[2:] + bits[:2],
    )


def product_rows(left, right):
    def part(start, count):
        return jnp.einsum(
            "tr,tc->rc",
            lax.dynamic_slice_in_dim(left, start, count, axis=1),
            right,
            preferred_element_type=jnp.float32,
        )

    return part


def sum_split(left, right, orders):
    rows = left.shape[1] // len(orders)
    done = []
    for place, order in enumerate(orders):
        columns = left[:, place * rows : (place + 1) * rows]
        done.append(sum_rows(product_rows(columns, right), rows, order, "dp"))
    return jnp.concatenate(done, axis=0) if len(done) > 1 else done[0]


def layer_norm(inputs, gain_row, shift_row):
    center = inputs - jnp.mean(inputs, axis=-1, keepdims=True)
    spread = jnp.mean(center * center, axis=-1, keepdims=True)
    return center * lax.rsqrt(spread + 1e-06) * gain_row + shift_row


def exact_gelu(inputs):
    return jax.nn.gelu(inputs, approximate=False)


def token_layout(classes, interp_index, interp_weight, row_count):
    image_count = classes.shape[0]
    lengths = POS + (LONG - POS) * classes
    image_ends = jnp.cumsum(lengths)
    image_starts = image_ends - lengths
    places = jnp.arange(row_count, dtype=jnp.int32)
    segment = jnp.sum((places[:, None] >= image_ends[None, :]).astype(jnp.int32), axis=1)
    member = segment[:, None] == jnp.arange(image_count, dtype=jnp.int32)[None, :]
    offset = places - jnp.sum(jnp.where(member, image_starts[None, :], 0), axis=1)
    is_long = jnp.sum(jnp.where(member, classes[None, :], 0), axis=1)
    in_image = segment < image_count
    weight_float = interp_weight.astype(jnp.float32)
    weight_share = weight_float / jnp.sum(weight_float, axis=1, keepdims=True)
    table_rows = jnp.arange(POS, dtype=jnp.int32)
    long_map = jnp.sum(
        weight_share[:, :, None]
        * (interp_index[:, :, None] == table_rows[None, None, :]).astype(jnp.float32),
        axis=1,
    )
    short_pick = (
        (offset[:, None] == table_rows[None, :]) & in_image[:, None] & (is_long[:, None] == 0)
    ).astype(jnp.float32)
    long_places = jnp.arange(LONG, dtype=jnp.int32)
    long_pick = (
        (offset[:, None] == long_places[None, :]) & in_image[:, None] & (is_long[:, None] == 1)
    ).astype(jnp.float32)
    mixing = short_pick + jnp.dot(long_pick, long_map, precision=lax.Precision.HIGHEST)
    return (mixing, segment)


def masked_scores(queries, keys_all, same_image, score_scale):
    scores = (
        jnp.einsum("qhd,khd->hqk", queries, keys_all, preferred_element_type=jnp.float32)
        * score_scale
    )
    return jnp.where(same_image[None], scores, -1000000000.0)


def shards(
    tokens,
    image_class,
    interp_index,
    interp_weight,
    position_table,
    norm_gain,
    norm_shift,
    attn_in_weight,
    attn_in_bias,
    attn_out_weight,
    attn_out_bias,
    up_weight,
    up_bias,
    down_weight,
    down_bias,
    cotangent,
):
    highest = lax.Precision.HIGHEST
    row_count = tokens.shape[0]
    mixing, segment = token_layout(image_class, interp_index, interp_weight, row_count)
    same_image = segment[:, None] == segment[None, :]
    score_scale = HD ** (-0.5)
    gains = norm_gain.astype(jnp.float32)
    shifts = norm_shift.astype(jnp.float32)
    residual_in = tokens.astype(jnp.float32) + jnp.dot(
        mixing, position_table.astype(jnp.float32), precision=highest
    )
    normed_one, norm_back_one = jax.vjp(layer_norm, residual_in, gains[0], shifts[0])
    first_low = normed_one.astype(jnp.bfloat16)
    projected = jnp.einsum(
        "td,cde->cte", first_low, attn_in_weight, preferred_element_type=jnp.float32
    )
    in_bias = attn_in_bias.astype(jnp.float32)
    projected = (
        projected + jnp.stack([in_bias[0], jnp.zeros_like(in_bias[0]), in_bias[1]])[:, None, :]
    )
    proj_low = projected.astype(jnp.bfloat16)
    width_here = proj_low.shape[2]
    heads_here = width_here // HD
    queries = proj_low[0].reshape(row_count, heads_here, HD)
    keys_all = proj_low[1].reshape(row_count, heads_here, HD)
    values_all = proj_low[2].reshape(row_count, heads_here, HD)
    scores = masked_scores(queries, keys_all, same_image, score_scale)
    row_peak = jnp.max(scores, axis=-1, keepdims=True)
    logsum = row_peak + jnp.log(jnp.sum(jnp.exp(scores - row_peak), axis=-1, keepdims=True))
    probs_low = jnp.exp(scores - logsum).astype(jnp.bfloat16)
    attended = jnp.einsum("hqk,khd->qhd", probs_low, values_all, preferred_element_type=jnp.float32)
    attended = attended.reshape(row_count, width_here).astype(jnp.bfloat16)
    attn_part = jnp.dot(attended, attn_out_weight, preferred_element_type=jnp.float32)
    middle = residual_in + sum_over(attn_part, "mp") + attn_out_bias.astype(jnp.float32)
    normed_two, norm_back_two = jax.vjp(layer_norm, middle, gains[1], shifts[1])
    second_low = normed_two.astype(jnp.bfloat16)
    hidden_pre = jnp.dot(
        second_low, up_weight, preferred_element_type=jnp.float32
    ) + up_bias.astype(jnp.float32)
    activ, gelu_back = jax.vjp(exact_gelu, hidden_pre)
    activ_low = activ.astype(jnp.bfloat16)
    mlp_part = jnp.dot(activ_low, down_weight, preferred_element_type=jnp.float32)
    block_out = (middle + sum_over(mlp_part, "mp") + down_bias.astype(jnp.float32)).astype(
        jnp.bfloat16
    )
    grad_final = cotangent.astype(jnp.float32)
    grad_down_bias = jnp.sum(grad_final, axis=0)
    orders = orders_of(lax.axis_size("dp"))
    grad_down_proj = sum_split(activ_low, cotangent, orders[:2])
    grad_activ = jnp.einsum("td,fd->tf", cotangent, down_weight, preferred_element_type=jnp.float32)
    grad_pre = gelu_back(grad_activ)[0].astype(jnp.bfloat16)
    grad_up_bias = jnp.sum(grad_pre.astype(jnp.float32), axis=0)
    grad_up_proj = sum_split(second_low, grad_pre, orders[:2])
    two_part = jnp.einsum("tf,df->td", grad_pre, up_weight, preferred_element_type=jnp.float32)
    grad_two = sum_over(two_part, "mp")
    back_middle, grad_gain_two, grad_shift_two = norm_back_two(grad_two)
    grad_middle = grad_final + back_middle
    grad_out_bias = jnp.sum(grad_middle, axis=0)
    middle_low = grad_middle.astype(jnp.bfloat16)
    grad_attn_out = sum_split(attended, middle_low, orders[2:])
    grad_attended = jnp.einsum(
        "td,cd->tc", middle_low, attn_out_weight, preferred_element_type=jnp.float32
    )
    grad_attended = grad_attended.astype(jnp.bfloat16).reshape(row_count, heads_here, HD)
    probs = jnp.exp(masked_scores(queries, keys_all, same_image, score_scale) - logsum)
    grad_values = jnp.einsum(
        "hqk,qhd->khd",
        probs.astype(jnp.bfloat16),
        grad_attended,
        preferred_element_type=jnp.float32,
    ).astype(jnp.bfloat16)
    grad_probs = jnp.einsum(
        "qhd,khd->hqk", grad_attended, values_all, preferred_element_type=jnp.float32
    )
    grad_scores = (
        probs * (grad_probs - jnp.sum(probs * grad_probs, axis=-1, keepdims=True))
    ).astype(jnp.bfloat16)
    grad_queries = (
        jnp.einsum("hqk,khd->qhd", grad_scores, keys_all, preferred_element_type=jnp.float32)
        * score_scale
    ).astype(jnp.bfloat16)
    grad_keys = (
        jnp.einsum("hqk,qhd->khd", grad_scores, queries, preferred_element_type=jnp.float32)
        * score_scale
    ).astype(jnp.bfloat16)
    grad_proj = jnp.stack(
        [
            grad_queries.reshape(row_count, width_here),
            grad_keys.reshape(row_count, width_here),
            grad_values.reshape(row_count, width_here),
        ]
    )
    grad_attn_in = jnp.stack(
        [sum_split(first_low, grad_proj[part], [orders[part % 3]]) for part in range(3)]
    )
    grad_in_bias = jnp.stack(
        [
            jnp.sum(grad_proj[0].astype(jnp.float32), axis=0),
            jnp.sum(grad_proj[2].astype(jnp.float32), axis=0),
        ]
    )
    one_part = jnp.einsum(
        "cte,cde->td", grad_proj, attn_in_weight, preferred_element_type=jnp.float32
    )
    grad_one = sum_over(one_part, "mp")
    back_residual, grad_gain_one, grad_shift_one = norm_back_one(grad_one)
    grad_inputs = grad_middle + back_residual
    grad_table = jnp.einsum("tp,td->pd", mixing, grad_inputs, precision=highest)
    width = tokens.shape[1]
    small = [
        grad_table,
        jnp.stack([grad_gain_one, grad_gain_two]),
        jnp.stack([grad_shift_one, grad_shift_two]),
        grad_out_bias,
        grad_down_bias,
        grad_up_bias,
        grad_in_bias,
    ]
    flat = jnp.concatenate([item.reshape(-1) for item in small])
    step = lax.axis_size("dp") * width
    flat = jnp.pad(flat, (0, -flat.shape[0] % step)).reshape(-1, width)
    flat = sum_rows(
        lambda start, count: lax.dynamic_slice_in_dim(flat, start, count),
        flat.shape[0],
        orders[0],
        "dp",
    ).reshape(-1)
    small_done = []
    place = 0
    for item in small:
        small_done.append(flat[place : place + item.size].reshape(item.shape))
        place += item.size
    return (
        block_out,
        grad_inputs,
        small_done[0],
        small_done[1],
        small_done[2],
        grad_attn_in,
        small_done[6],
        grad_attn_out,
        small_done[3],
        grad_up_proj,
        small_done[5],
        grad_down_proj,
        small_done[4],
    )


def solution(mesh):
    return jax.shard_map(
        shards,
        mesh=mesh,
        in_specs=(
            P("dp", None),
            P("dp"),
            P(),
            P(),
            P(),
            P(),
            P(),
            P(None, None, "mp"),
            P(None, "mp"),
            P("mp", None),
            P(),
            P(None, "mp"),
            P("mp"),
            P("mp", None),
            P(),
            P("dp", None),
        ),
        out_specs=(
            P("dp", None),
            P("dp", None),
            P(),
            P(),
            P(),
            P(None, None, "mp"),
            P(None, "mp"),
            P("mp", None),
            P(),
            P(None, "mp"),
            P("mp"),
            P("mp", None),
            P(),
        ),
        check_vma=False,
    )
```

```python
import functools

import jax
import jax.numpy as jnp
from jax import lax
from jax.experimental import pallas as pl
from jax.experimental.pallas import tpu as pltpu
from jax.sharding import PartitionSpec as P

HD = 64
POS = 50
LONG = 145
BLOCK = 128
PAIR = 128
MASKED = -1000000000.0


def log_two(size):
    return size.bit_length() - 1


def swap_pairs(size, bit):
    return [(index, index ^ (1 << bit)) for index in range(size)]


def sum_over(value, axis):
    size = lax.axis_size(axis)
    if size & (size - 1):
        return lax.psum(value, axis)
    for bit in range(log_two(size)):
        value = value + lax.ppermute(value, axis, swap_pairs(size, bit))
    return value


def bit_of(axis, bit):
    return (lax.axis_index(axis) >> bit) & 1


def begin_sum(part, rows, order, axis):
    half = rows // 2
    first = bit_of(axis, order[0])
    sent = part((1 - first) * half, half)
    arrived = lax.ppermute(sent, axis, swap_pairs(lax.axis_size(axis), order[0]))
    held = part(first * half, half)
    return held, arrived


def finish_sum(pair, order, axis, target=None, place=0):
    size = lax.axis_size(axis)
    held, arrived = pair
    half = held.shape[0]
    for bit in order[1:]:
        half = half // 2
        here = bit_of(axis, bit)
        away = (1 - here) * half
        mine = here * half
        sent = lax.dynamic_slice_in_dim(held, away, half) + lax.dynamic_slice_in_dim(
            arrived, away, half
        )
        arrived_next = lax.ppermute(sent, axis, swap_pairs(size, bit))
        held = lax.dynamic_slice_in_dim(held, mine, half) + lax.dynamic_slice_in_dim(
            arrived, mine, half
        )
        arrived = arrived_next
    held = held + arrived
    for bit in reversed(order[1:]):
        other = lax.ppermute(held, axis, swap_pairs(size, bit))
        here = bit_of(axis, bit)
        held = jnp.where(
            here == 0,
            jnp.concatenate([held, other], axis=0),
            jnp.concatenate([other, held], axis=0),
        )
    other = lax.ppermute(held, axis, swap_pairs(size, order[0]))
    here = bit_of(axis, order[0])
    half = held.shape[0]
    if target is None:
        return jnp.where(
            here == 0,
            jnp.concatenate([held, other], axis=0),
            jnp.concatenate([other, held], axis=0),
        )
    target = lax.dynamic_update_slice_in_dim(target, held, place + here * half, 0)
    return lax.dynamic_update_slice_in_dim(target, other, place + (1 - here) * half, 0)


def orders_of(size):
    bits = list(range(log_two(size)))
    return (
        bits,
        [bits[1], bits[0]] + bits[2:],
        bits[2:] + bits[:2],
    )


def product_rows(left, right, first_row):
    def part(start, count):
        return jnp.einsum(
            "tr,tc->rc",
            lax.dynamic_slice_in_dim(left, first_row + start, count, axis=1),
            right,
            preferred_element_type=jnp.float32,
        )

    return part


def begin_product(left, right, cuts):
    chunks = []
    place = 0
    for rows, order in cuts:
        pair = begin_sum(product_rows(left, right, place), rows, order, "dp")
        chunks.append((pair, order, place))
        place += rows
    return chunks


def finish_product(chunks, rows, columns):
    target = jnp.zeros((rows, columns), jnp.float32)
    for pair, order, place in chunks:
        target = finish_sum(pair, order, "dp", target, place)
    return target


def layer_norm(inputs, gain_row, shift_row):
    center = inputs - jnp.mean(inputs, axis=-1, keepdims=True)
    spread = jnp.mean(center * center, axis=-1, keepdims=True)
    return center * lax.rsqrt(spread + 1e-06) * gain_row + shift_row


def token_layout(classes, interp_index, interp_weight, row_count):
    image_count = classes.shape[0]
    lengths = POS + (LONG - POS) * classes
    image_ends = jnp.cumsum(lengths)
    image_starts = image_ends - lengths
    places = jnp.arange(row_count, dtype=jnp.int32)
    segment = jnp.sum((places[:, None] >= image_ends[None, :]).astype(jnp.int32), axis=1)
    member = segment[:, None] == jnp.arange(image_count, dtype=jnp.int32)[None, :]
    offset = places - jnp.sum(jnp.where(member, image_starts[None, :], 0), axis=1)
    is_long = jnp.sum(jnp.where(member, classes[None, :], 0), axis=1)
    in_image = segment < image_count
    weight_float = interp_weight.astype(jnp.float32)
    weight_share = weight_float / jnp.sum(weight_float, axis=1, keepdims=True)
    table_rows = jnp.arange(POS, dtype=jnp.int32)
    long_map = jnp.sum(
        weight_share[:, :, None]
        * (interp_index[:, :, None] == table_rows[None, None, :]).astype(jnp.float32),
        axis=1,
    )
    short_pick = (
        (offset[:, None] == table_rows[None, :]) & in_image[:, None] & (is_long[:, None] == 0)
    ).astype(jnp.float32)
    long_places = jnp.arange(LONG, dtype=jnp.int32)
    long_pick = (
        (offset[:, None] == long_places[None, :]) & in_image[:, None] & (is_long[:, None] == 1)
    ).astype(jnp.float32)
    mixing = short_pick + jnp.dot(long_pick, long_map, precision=lax.Precision.HIGHEST)
    return (mixing, segment)


def key_range(segment, row_count):
    blocks = row_count // BLOCK
    first = segment[::BLOCK]
    last = segment[BLOCK - 1 :: BLOCK]
    low = jnp.sum((segment[None, :] < first[:, None]).astype(jnp.int32), axis=1)
    high = jnp.sum((segment[None, :] <= last[:, None]).astype(jnp.int32), axis=1)
    return jnp.concatenate([low // BLOCK, (high + BLOCK - 1) // BLOCK]).astype(jnp.int32).reshape(2, blocks)


NT = (((1,), (1,)), ((), ()))
NN = (((1,), (0,)), ((), ()))
TN = (((0,), (0,)), ((), ()))


def mul(left, right, dims):
    return lax.dot_general(left, right, dims, preferred_element_type=jnp.float32)


def half_lanes(value, head):
    lane = lax.broadcasted_iota(jnp.int32, value.shape, 1)
    keep = (lane >= HD) if head % 2 else (lane < HD)
    return jnp.where(keep, value, jnp.zeros_like(value))


def attend_kernel(range_ref, qkv_ref, column_ref, row_ref, out_ref, log_ref, held, peak, total):
    step = pl.program_id(0)
    width = qkv_ref.shape[1] // 3
    heads = width // HD
    rows = pl.ds(pl.multiple_of(step * BLOCK, BLOCK), BLOCK)
    low, high = range_ref[0, step], range_ref[1, step]
    queries = [
        half_lanes(
            qkv_ref[rows, (head // 2) * PAIR : (head // 2 + 1) * PAIR] * jnp.bfloat16(HD**-0.5),
            head,
        )
        for head in range(heads)
    ]
    row_segment = row_ref[0:1, rows]
    peak[...] = jnp.full(peak.shape, 2.0 * MASKED, jnp.float32)
    total[...] = jnp.zeros(total.shape, jnp.float32)

    def key_rows(block):
        return pl.ds(pl.multiple_of(block * BLOCK, BLOCK), BLOCK)

    def score(block, carry):
        there = key_rows(block)
        same = column_ref[there, :] == row_segment
        for head in range(heads):
            pair = head // 2
            keys = qkv_ref[there, width + pair * PAIR : width + (pair + 1) * PAIR]
            scores = jnp.where(same, mul(keys, queries[head], NT), MASKED)
            held[block, head] = scores
            peak[head : head + 1, :] = jnp.maximum(
                peak[head : head + 1, :], jnp.max(scores, axis=0, keepdims=True)
            )
        return carry

    lax.fori_loop(low, high, score, 0)

    def weigh(block, carry):
        for head in range(heads):
            weights = jnp.exp(held[block, head] - peak[head : head + 1, :])
            held[block, head] = weights
            total[head : head + 1, :] += jnp.sum(weights, axis=0, keepdims=True)
        return carry

    lax.fori_loop(low, high, weigh, 0)
    log_ref[...] = peak[...] + jnp.log(total[...])
    total[...] = 1.0 / total[...]
    out = []

    def gather(block, sums):
        there = key_rows(block)
        new = []
        for head in range(heads):
            pair = head // 2
            values = qkv_ref[there, 2 * width + pair * PAIR : 2 * width + (pair + 1) * PAIR]
            probs = (held[block, head] * total[head : head + 1, :]).astype(jnp.bfloat16)
            part = mul(probs, half_lanes(values, head), TN)
            if head % 2:
                new[pair] = new[pair] + part
            else:
                new.append(sums[pair] + part)
        return tuple(new)

    sums = lax.fori_loop(
        low,
        high,
        gather,
        tuple(jnp.zeros((BLOCK, PAIR), jnp.float32) for _ in range(heads // 2)),
    )
    for pair in range(heads // 2):
        out_ref[:, pair * PAIR : (pair + 1) * PAIR] = sums[pair].astype(jnp.bfloat16)


def attend(ranges, qkv, column, row):
    row_count, triple = qkv.shape
    width = triple // 3
    heads = width // HD
    blocks = row_count // BLOCK
    return pl.pallas_call(
        attend_kernel,
        out_shape=(
            jax.ShapeDtypeStruct((row_count, width), jnp.bfloat16),
            jax.ShapeDtypeStruct((heads, row_count), jnp.float32),
        ),
        grid_spec=pltpu.PrefetchScalarGridSpec(
            num_scalar_prefetch=1,
            grid=(blocks,),
            in_specs=[
                pl.BlockSpec((row_count, triple), lambda i, r: (0, 0)),
                pl.BlockSpec((row_count, PAIR), lambda i, r: (0, 0)),
                pl.BlockSpec((8, row_count), lambda i, r: (0, 0)),
            ],
            out_specs=(
                pl.BlockSpec((BLOCK, width), lambda i, r: (i, 0)),
                pl.BlockSpec((heads, BLOCK), lambda i, r: (0, i)),
            ),
            scratch_shapes=[
                pltpu.VMEM((blocks, heads, BLOCK, BLOCK), jnp.float32),
                pltpu.VMEM((heads, BLOCK), jnp.float32),
                pltpu.VMEM((heads, BLOCK), jnp.float32),
            ],
        ),
        cost_estimate=pl.CostEstimate(
            flops=4 * row_count * 3 * BLOCK * width * 2,
            bytes_accessed=8 * row_count * width,
            transcendentals=row_count * 3 * BLOCK * heads,
        ),
        name="attend",
    )(ranges, qkv, column, row)


def attend_back_kernel(
    range_ref, qkv_ref, grad_ref, log_ref, column_ref, row_ref, out_ref, held, slope, inner, sums
):
    step = pl.program_id(0)
    width = qkv_ref.shape[1] // 3
    heads = width // HD
    rows = pl.ds(pl.multiple_of(step * BLOCK, BLOCK), BLOCK)
    low, high = range_ref[0, step], range_ref[1, step]
    scale = jnp.bfloat16(HD**-0.5)
    row_segment = row_ref[0:1, rows]

    @pl.when(step == 0)
    def _():
        sums[...] = jnp.zeros(sums.shape, jnp.float32)

    inner[...] = jnp.zeros(inner.shape, jnp.float32)
    queries = [
        half_lanes(qkv_ref[rows, (head // 2) * PAIR : (head // 2 + 1) * PAIR] * scale, head)
        for head in range(heads)
    ]
    grads = [
        half_lanes(grad_ref[:, (head // 2) * PAIR : (head // 2 + 1) * PAIR], head)
        for head in range(heads)
    ]

    def key_rows(block):
        return pl.ds(pl.multiple_of(block * BLOCK, BLOCK), BLOCK)

    def score(block, carry):
        there = key_rows(block)
        same = column_ref[there, :] == row_segment
        for pair in range(heads // 2):
            lanes = slice(pair * PAIR, (pair + 1) * PAIR)
            keys = qkv_ref[there, width + pair * PAIR : width + (pair + 1) * PAIR]
            values = qkv_ref[there, 2 * width + pair * PAIR : 2 * width + (pair + 1) * PAIR]
            grad_values = sums[1, there, lanes]
            for head in (2 * pair, 2 * pair + 1):
                scores = jnp.where(same, mul(keys, queries[head], NT), MASKED)
                probs = jnp.exp(scores - log_ref[head : head + 1, :])
                grad_probs = mul(values, grads[head], NT)
                grad_values = grad_values + mul(probs.astype(jnp.bfloat16), grads[head], NN)
                held[block, head] = probs
                slope[block, head] = grad_probs
                inner[head : head + 1, :] += jnp.sum(probs * grad_probs, axis=0, keepdims=True)
            sums[1, there, lanes] = grad_values
        return carry

    lax.fori_loop(low, high, score, 0)

    def gather(block, carry):
        there = key_rows(block)
        new = []
        for pair in range(heads // 2):
            lanes = slice(pair * PAIR, (pair + 1) * PAIR)
            keys = qkv_ref[there, width + pair * PAIR : width + (pair + 1) * PAIR] * scale
            grad_keys = sums[0, there, lanes]
            total = carry[pair]
            for head in (2 * pair, 2 * pair + 1):
                grad_scores = (
                    held[block, head] * (slope[block, head] - inner[head : head + 1, :])
                ).astype(jnp.bfloat16)
                grad_keys = grad_keys + mul(grad_scores, queries[head], NN)
                total = total + mul(grad_scores, half_lanes(keys, head), TN)
            sums[0, there, lanes] = grad_keys
            new.append(total)
        return tuple(new)

    totals = lax.fori_loop(
        low,
        high,
        gather,
        tuple(jnp.zeros((BLOCK, PAIR), jnp.float32) for _ in range(heads // 2)),
    )
    for pair in range(heads // 2):
        out_ref[rows, pair * PAIR : (pair + 1) * PAIR] = totals[pair].astype(jnp.bfloat16)

    @pl.when(step == pl.num_programs(0) - 1)
    def _():
        def put(block, carry):
            there = key_rows(block)
            out_ref[there, width : 2 * width] = sums[0, there, :].astype(jnp.bfloat16)
            out_ref[there, 2 * width : 3 * width] = sums[1, there, :].astype(jnp.bfloat16)
            return carry

        lax.fori_loop(0, out_ref.shape[0] // BLOCK, put, 0)


def attend_back(ranges, qkv, grad_attended, logsum, column, row):
    row_count, triple = qkv.shape
    width = triple // 3
    heads = width // HD
    blocks = row_count // BLOCK
    return pl.pallas_call(
        attend_back_kernel,
        out_shape=jax.ShapeDtypeStruct((row_count, triple), jnp.bfloat16),
        grid_spec=pltpu.PrefetchScalarGridSpec(
            num_scalar_prefetch=1,
            grid=(blocks,),
            in_specs=[
                pl.BlockSpec((row_count, triple), lambda i, r: (0, 0)),
                pl.BlockSpec((BLOCK, width), lambda i, r: (i, 0)),
                pl.BlockSpec((heads, BLOCK), lambda i, r: (0, i)),
                pl.BlockSpec((row_count, PAIR), lambda i, r: (0, 0)),
                pl.BlockSpec((8, row_count), lambda i, r: (0, 0)),
            ],
            out_specs=pl.BlockSpec((row_count, triple), lambda i, r: (0, 0)),
            scratch_shapes=[
                pltpu.VMEM((blocks, heads, BLOCK, BLOCK), jnp.float32),
                pltpu.VMEM((blocks, heads, BLOCK, BLOCK), jnp.float32),
                pltpu.VMEM((heads, BLOCK), jnp.float32),
                pltpu.VMEM((2, row_count, width), jnp.float32),
            ],
        ),
        cost_estimate=pl.CostEstimate(
            flops=10 * row_count * 3 * BLOCK * width * 2,
            bytes_accessed=14 * row_count * width,
            transcendentals=row_count * 3 * BLOCK * heads,
        ),
        name="attend_back",
    )(ranges, qkv, grad_attended, logsum, column, row)


def shards(
    tokens,
    image_class,
    interp_index,
    interp_weight,
    position_table,
    norm_gain,
    norm_shift,
    attn_in_weight,
    attn_in_bias,
    attn_out_weight,
    attn_out_bias,
    up_weight,
    up_bias,
    down_weight,
    down_bias,
    cotangent,
):
    highest = lax.Precision.HIGHEST
    row_count, features = tokens.shape
    hidden_here = up_weight.shape[1]
    width_here = attn_out_weight.shape[0]
    mixing, segment = token_layout(image_class, interp_index, interp_weight, row_count)
    ranges = key_range(segment, row_count)
    column = jnp.broadcast_to(segment[:, None], (row_count, PAIR))
    row = jnp.broadcast_to(segment[None, :], (8, row_count))
    gains = norm_gain.astype(jnp.float32)
    shifts = norm_shift.astype(jnp.float32)
    orders = orders_of(lax.axis_size("dp"))
    residual_in = tokens.astype(jnp.float32) + jnp.dot(
        mixing, position_table.astype(jnp.float32), precision=highest
    )
    normed_one, norm_back_one = jax.vjp(layer_norm, residual_in, gains[0], shifts[0])
    first_low = normed_one.astype(jnp.bfloat16)
    in_weight = jnp.concatenate([attn_in_weight[0], attn_in_weight[1], attn_in_weight[2]], axis=1)
    in_bias = attn_in_bias.astype(jnp.float32)
    wide_bias = jnp.concatenate([in_bias[0], jnp.zeros_like(in_bias[0]), in_bias[1]])
    qkv = (
        jnp.dot(first_low, in_weight, preferred_element_type=jnp.float32) + wide_bias[None, :]
    ).astype(jnp.bfloat16)
    attended, logsum = attend(ranges, qkv, column, row)
    attn_part = jnp.dot(attended, attn_out_weight, preferred_element_type=jnp.float32)
    middle = residual_in + sum_over(attn_part, "mp") + attn_out_bias.astype(jnp.float32)
    normed_two, norm_back_two = jax.vjp(layer_norm, middle, gains[1], shifts[1])
    second_low = normed_two.astype(jnp.bfloat16)
    hidden_pre = jnp.dot(
        second_low, up_weight, preferred_element_type=jnp.float32
    ) + up_bias.astype(jnp.float32)
    below = 0.5 * (1.0 + lax.erf(hidden_pre * (0.5**0.5)))
    activ_low = (hidden_pre * below).astype(jnp.bfloat16)
    gelu_slope = below + hidden_pre * (
        jnp.exp(-0.5 * hidden_pre * hidden_pre) * 0.3989422804014327
    )
    activ_low, gelu_slope = lax.optimization_barrier((activ_low, gelu_slope))
    half_hidden = hidden_here // 2
    down_chunks = begin_product(
        activ_low, cotangent, [(half_hidden, orders[0]), (half_hidden, orders[1])]
    )
    grad_activ = jnp.einsum("td,fd->tf", cotangent, down_weight, preferred_element_type=jnp.float32)
    grad_pre = (grad_activ * gelu_slope).astype(jnp.bfloat16)
    up_chunks = begin_product(
        second_low, grad_pre, [(features // 2, orders[0]), (features // 2, orders[1])]
    )
    two_part = jnp.einsum("tf,df->td", grad_pre, up_weight, preferred_element_type=jnp.float32)
    grad_final = cotangent.astype(jnp.float32)
    grad_two = sum_over(two_part, "mp")
    back_middle, grad_gain_two, grad_shift_two = norm_back_two(grad_two)
    grad_middle = grad_final + back_middle
    grad_out_bias = jnp.sum(grad_middle, axis=0)
    middle_low = grad_middle.astype(jnp.bfloat16)
    grad_attended = jnp.einsum(
        "td,cd->tc", middle_low, attn_out_weight, preferred_element_type=jnp.float32
    ).astype(jnp.bfloat16)
    grad_qkv = attend_back(ranges, qkv, grad_attended, logsum, column, row)
    out_chunks = begin_product(attended, middle_low, [(width_here, orders[2])])
    in_chunks = begin_product(
        first_low,
        grad_qkv,
        [
            (3 * features // 8, orders[0]),
            (3 * features // 8, orders[1]),
            (features // 4, orders[2]),
        ],
    )
    mlp_part = jnp.dot(activ_low, down_weight, preferred_element_type=jnp.float32)
    block_out = (middle + sum_over(mlp_part, "mp") + down_bias.astype(jnp.float32)).astype(
        jnp.bfloat16
    )
    pairs = [chunk[0] for chunk in down_chunks + up_chunks]
    pairs, grad_qkv = lax.optimization_barrier((pairs, grad_qkv))
    down_chunks = [(pair,) + chunk[1:] for pair, chunk in zip(pairs[:2], down_chunks)]
    up_chunks = [(pair,) + chunk[1:] for pair, chunk in zip(pairs[2:], up_chunks)]
    grad_down_bias = jnp.sum(grad_final, axis=0)
    grad_up_bias = jnp.sum(grad_pre.astype(jnp.float32), axis=0)
    grad_wide_bias = jnp.sum(grad_qkv.astype(jnp.float32), axis=0)
    grad_in_bias = jnp.stack([grad_wide_bias[:width_here], grad_wide_bias[2 * width_here :]])
    one_part = jnp.einsum("te,de->td", grad_qkv, in_weight, preferred_element_type=jnp.float32)
    grad_one = sum_over(one_part, "mp")
    back_residual, grad_gain_one, grad_shift_one = norm_back_one(grad_one)
    grad_inputs = grad_middle + back_residual
    grad_table = jnp.einsum("tp,td->pd", mixing, grad_inputs, precision=highest)
    small = [
        grad_table,
        jnp.stack([grad_gain_one, grad_gain_two]),
        jnp.stack([grad_shift_one, grad_shift_two]),
        grad_out_bias,
        grad_down_bias,
        grad_up_bias,
        grad_in_bias,
    ]
    flat = jnp.concatenate([item.reshape(-1) for item in small])
    flat = jnp.pad(flat, (0, -flat.shape[0] % (lax.axis_size("dp") * features)))
    flat = flat.reshape(-1, features)
    flat_pair = begin_sum(
        lambda start, count: lax.dynamic_slice_in_dim(flat, start, count),
        flat.shape[0],
        orders[2],
        "dp",
    )
    grad_down_proj = finish_product(down_chunks, hidden_here, features)
    grad_up_proj = finish_product(up_chunks, features, hidden_here)
    grad_attn_out = finish_product(out_chunks, width_here, features)
    grad_wide = finish_product(in_chunks, features, 3 * width_here)
    grad_attn_in = jnp.stack(
        [grad_wide[:, part * width_here : (part + 1) * width_here] for part in range(3)]
    )
    flat = finish_sum(flat_pair, orders[2], "dp").reshape(-1)
    small_done = []
    place = 0
    for item in small:
        small_done.append(flat[place : place + item.size].reshape(item.shape))
        place += item.size
    return (
        block_out,
        grad_inputs,
        small_done[0],
        small_done[1],
        small_done[2],
        grad_attn_in,
        small_done[6],
        grad_attn_out,
        small_done[3],
        grad_up_proj,
        small_done[5],
        grad_down_proj,
        small_done[4],
    )


def solution(mesh):
    return jax.shard_map(
        shards,
        mesh=mesh,
        in_specs=(
            P("dp", None),
            P("dp"),
            P(),
            P(),
            P(),
            P(),
            P(),
            P(None, None, "mp"),
            P(None, "mp"),
            P("mp", None),
            P(),
            P(None, "mp"),
            P("mp"),
            P("mp", None),
            P(),
            P("dp", None),
        ),
        out_specs=(
            P("dp", None),
            P("dp", None),
            P(),
            P(),
            P(),
            P(None, None, "mp"),
            P(None, "mp"),
            P("mp", None),
            P(),
            P(None, "mp"),
            P("mp"),
            P("mp", None),
            P(),
        ),
        check_vma=False,
    )
```
